1024 devices in a mesh: dp: 16 (over x, core), expert: 64 (over z, y).
Axes of the slice: x: 8, y: 8, z: 8, core: 2. Of those that a mesh axis runs over, the one named last changes fastest.
Arguments:
- tokens: bfloat16 [16384, 2048], P(('dp', 'expert')), may hold values from -24 to 24
- out_grad: bfloat16 [16384, 2048], P(('dp', 'expert')), may hold values from -24 to 24
- expert_ids: int32 [16384, 8], P(('dp', 'expert')), may hold values from 0 to 63, all different within a row; in each aligned block of 16 rows (0 to 15, 16 to 31, ...) at most 4 rows name the same one
- probs: bfloat16 [16384, 8], P(('dp', 'expert')), may hold values from 0.049804688 to 0.5
- w_gate: bfloat16 [64, 2048, 384], P('expert'), may hold values from -0.125 to 0.125
- w_up: bfloat16 [64, 2048, 384], P('expert'), may hold values from -0.125 to 0.125
- w_down: bfloat16 [64, 2048, 384], P('expert'), may hold values from -0.3125 to 0.3125
Outputs:
- token_grad: bfloat16 [16384, 2048], P(('dp', 'expert'))
- prob_grad: bfloat16 [16384, 8], P(('dp', 'expert'))
- gate_grad: float32 [64, 2048, 384], P('expert', 'dp')
- up_grad: float32 [64, 2048, 384], P('expert', 'dp')
- down_grad: float32 [64, 2048, 384], P('expert', 'dp')
The draws below stay inside these ranges and needn't reach their ends.
Inputs may be any that keep to these rules, and one draw needn't show every extreme that they name: `expert_ids`: each row names 8 different experts. Within each aligned block of 16 rows (the rows of one device) no expert is named by more than 4 rows, and that bound is reached in some blocks.
All inputs are finite; a program needn't handle non-finite values.
Results may differ from the reference program's by a relative error of at most 0.017.
Values may be sent and summed in bfloat16 or wider, within the bound.
A program may use at most 64 MiB of HBM per device.

```python
import math
import jax
import jax.numpy as jnp
import numpy as np
from jax import lax

D = 2048
FF = 384
EXPERTS = 64
TOP = 8
TOK_DEV = 16
CAP = 4
TOKENS = 16384
N_DP = 16
N_EXPERT = 64


def with_spikes(values, stream_key, source, target, blocks, factor):
    owner, partner = [(jnp.arange(values.shape[axis_at]) // (values.shape[axis_at] // blocks)).reshape([-1 if axis == axis_at else 1 for axis in range(values.ndim)]) for axis_at in (source, target)]
    chosen = jax.random.permutation(stream_key, blocks)[partner]
    strong = (owner == chosen) | (owner == (partner + blocks // 2) % blocks)
    return jnp.where(strong, factor * values, values)


def levels(key, dims, cuts, smallest, largest):
    gain, own = 1.0, jax.random.fold_in(key, 6)
    for position, shards_of in cuts:
        draws = jnp.exp(jax.random.uniform(jax.random.fold_in(own, position), (shards_of,), jnp.float32, smallest / len(cuts), largest / len(cuts)))
        gain = gain * jnp.repeat(draws, dims[position] // shards_of).reshape([-1 if axis == position else 1 for axis in range(len(dims))])
    return gain


def shared_out(key, own, number, rows, number_of, top, reach, slope):
    sequence = jax.random.permutation(key, number_of)
    packed, usual = load_shares(number_of, rows * top, reach, slope, True), load_shares(number_of, rows * top, reach, slope, False)
    places = jnp.arange(number_of)

    def named(tallies, offset_by):
        used = int((tallies > 0).sum())
        fixed = max(1, used // 4)
        passed = fixed + (places - fixed + offset_by * (used - fixed)) % max(1, number_of - fixed)
        return jnp.zeros((number_of,), jnp.int32).at[sequence[jnp.where(places < fixed, places, passed)]].set(jnp.asarray(tallies, jnp.int32))

    tallies = jnp.where(number % 4 == 0, named(packed, number // 4), named(usual, number - number // 4 - 1))
    mixed = jax.random.permutation(jax.random.fold_in(own, 3), number_of)
    source_of, receiver = mixed[0:number_of // 2 * 2:2], mixed[1:number_of // 2 * 2:2]
    margin = jnp.minimum(tallies[source_of] - 1, reach - tallies[receiver]) // 2
    margin = jnp.where((source_of == sequence[0]) | (receiver == sequence[0]) | (tallies[receiver] == 0), 0, jnp.maximum(margin, 0))
    passed = jax.random.randint(jax.random.fold_in(own, 4), (number_of // 2,), 0, 1 << 20) % (margin + 1)
    tallies = tallies.at[source_of].add(-passed).at[receiver].add(passed)
    items = jnp.searchsorted(jnp.cumsum(tallies), jnp.arange(rows * top), side="right").astype(jnp.int32)
    table = items.reshape(top, rows).T
    table = table[jax.random.permutation(jax.random.fold_in(own, 1), rows)]
    offset_by = jax.random.randint(jax.random.fold_in(own, 2), (rows, 1), 0, top)
    return jnp.take_along_axis(table, (jnp.arange(top)[None, :] + offset_by) % top, axis=1)


def load_shares(amount, total, most, skew, full):
    loads = [(1 << 20) // math.isqrt(rank ** skew) + 1 for rank in range(1, amount + 1)]
    largest = most if full else min(most, max(-(-total // amount), total * loads[0] // sum(loads)))
    least = 1 if total - largest >= amount - 1 else 0
    given, rest = [largest] + [least] * (amount - 1), total - largest - least * (amount - 1)
    while rest > 0:
        movable = [i for i in range(1, amount) if given[i] < largest] or [i for i in range(1, amount) if given[i] < most]
        mass, budget = sum([loads[i] for i in movable]), rest
        for i in movable:
            more = min(most - given[i], max(1, budget * loads[i] // mass), rest)
            given[i] = given[i] + more
            rest = rest - more
    return np.array(given)


def noise(stream_key, extent, width, limit, pieces=(), held_as=jnp.bfloat16):
    entries = jax.random.normal(stream_key, extent, jnp.float32) * width
    if len(pieces) > 0:
        entries = levels(stream_key, extent, pieces, -0.22, 0.18) * entries
    return jnp.clip(entries, min=-limit, max=limit).astype(held_as)


def heavy_noise(key, extent, scale, most, pieces, heavy, held_as=jnp.bfloat16):
    drawn = scale * jax.random.normal(key, extent, jnp.float32)
    if pieces:
        drawn = drawn * levels(key, extent, pieces, -0.22, 0.18)
    return jnp.clip(with_spikes(drawn, jax.random.fold_in(key, 3), *heavy), -most, most).astype(held_as)


def setup_inputs(seed: int = 0) -> dict:
    streams_of = jax.random.split(jax.random.key(seed), 8)
    tokens = heavy_noise(streams_of[0], (TOKENS, D), 1.0, 24.0, ((0, 1024),), (0, 1, 1024, 6.0))
    out_grad = heavy_noise(streams_of[1], (TOKENS, D), 1.0, 24.0, ((0, 1024),), (0, 1, 1024, 6.0))
    expert_ids_keys = jax.random.split(jax.random.fold_in(streams_of[2], 1), TOKENS // TOK_DEV)
    expert_ids_turns = jax.random.permutation(jax.random.fold_in(streams_of[2], 3), TOKENS // TOK_DEV)
    expert_ids = jax.vmap(lambda own, number: shared_out(jax.random.fold_in(streams_of[2], 2), own, number, TOK_DEV, EXPERTS, TOP, CAP, 1))(expert_ids_keys, expert_ids_turns).reshape((TOKENS, TOP))
    probs = jnp.clip(0.049804688 + 0.4501953 * jax.random.uniform(streams_of[3], (TOKENS, TOP), jnp.float32) ** levels(streams_of[3], (TOKENS, TOP), ((0, 1024),), -0.2, 0.2), 0.049804688, 0.5).astype(jnp.bfloat16)
    w_gate = noise(streams_of[4], (EXPERTS, D, FF), D ** -0.5, 0.125, ((0, 64),))
    w_up = noise(streams_of[5], (EXPERTS, D, FF), D ** -0.5, 0.125, ((0, 64),))
    w_down = noise(streams_of[6], (EXPERTS, D, FF), FF ** -0.5, 0.3125, ((0, 64),))
    return dict(tokens=tokens, out_grad=out_grad, expert_ids=expert_ids, probs=probs, w_gate=w_gate, w_up=w_up, w_down=w_down)


def slot_targets(ids):
    flat = ids.reshape(ids.shape[0], -1)
    onehot = (flat[:, :, None] == jnp.arange(EXPERTS, dtype=jnp.int32)[None, None, :]).astype(jnp.int32)
    before = jnp.cumsum(onehot, axis=1) - onehot
    place = jnp.sum(before * onehot, axis=2).astype(jnp.int32)
    return (flat * CAP + place).astype(jnp.int32)


def rounded(value):
    narrow = lax.optimization_barrier(value.astype(jnp.bfloat16))
    return narrow.astype(jnp.float32)


def expert_pass(inputs):
    rows_x, rows_dy, rows_p, weight_gate, weight_up, weight_down = inputs
    gate_pre = jnp.dot(rows_x, weight_gate, preferred_element_type=jnp.float32)
    up_pre = jnp.dot(rows_x, weight_up, preferred_element_type=jnp.float32)
    sigma = jax.nn.sigmoid(gate_pre)
    silu = gate_pre * sigma
    act = (silu * up_pre).astype(jnp.bfloat16)
    scaled = (rows_p.astype(jnp.float32)[:, None] * rows_dy.astype(jnp.float32)).astype(jnp.bfloat16)
    expert_out = jnp.dot(act, weight_down.T, preferred_element_type=jnp.float32)
    prob_back = jnp.sum(rows_dy.astype(jnp.float32) * expert_out, axis=1).astype(jnp.bfloat16)
    act_grad = jnp.dot(scaled, weight_down, preferred_element_type=jnp.float32)
    gate_back = (act_grad * up_pre * sigma * (1.0 + gate_pre * (1.0 - sigma))).astype(jnp.bfloat16)
    up_back = (act_grad * silu).astype(jnp.bfloat16)
    contrib = (jnp.dot(gate_back, weight_gate.T, preferred_element_type=jnp.float32)
               + jnp.dot(up_back, weight_up.T, preferred_element_type=jnp.float32)).astype(jnp.bfloat16)
    group_gate = rounded(jnp.dot(rows_x.T, gate_back, preferred_element_type=jnp.float32))
    group_up = rounded(jnp.dot(rows_x.T, up_back, preferred_element_type=jnp.float32))
    group_down = rounded(jnp.dot(scaled.T, act, preferred_element_type=jnp.float32))
    return contrib, prob_back, (group_gate, group_up, group_down)


def reference(tokens, out_grad, expert_ids, probs, w_gate, w_up, w_down):
    pairs = TOK_DEV * TOP
    token_of = jnp.arange(pairs, dtype=jnp.int32) // TOP
    source = jnp.arange(N_EXPERT, dtype=jnp.int32)[:, None]

    def to_experts(buffer):
        shape = buffer.shape[2:]
        grid = buffer.reshape((N_EXPERT, EXPERTS, CAP) + shape)
        grid = jnp.moveaxis(grid, 1, 0)
        return grid.reshape((EXPERTS, N_EXPERT * CAP) + shape)

    def from_experts(result):
        shape = result.shape[2:]
        grid = result.reshape((EXPERTS, N_EXPERT, CAP) + shape)
        grid = jnp.moveaxis(grid, 0, 1)
        return grid.reshape((N_EXPERT, EXPERTS * CAP) + shape)

    def group_pass(carry, group):
        group_x, group_dy, group_ids, group_p = group
        target = slot_targets(group_ids)
        rows_x = group_x[:, token_of]
        rows_dy = group_dy[:, token_of]
        buffer_x = jnp.zeros((N_EXPERT, EXPERTS * CAP, D), jnp.bfloat16).at[source, target].set(rows_x)
        buffer_dy = jnp.zeros((N_EXPERT, EXPERTS * CAP, D), jnp.bfloat16).at[source, target].set(rows_dy)
        buffer_p = jnp.zeros((N_EXPERT, EXPERTS * CAP), jnp.bfloat16).at[source, target].set(group_p.reshape(N_EXPERT, pairs))
        contrib, prob_back, grads = lax.map(expert_pass, (to_experts(buffer_x), to_experts(buffer_dy), to_experts(buffer_p), w_gate, w_up, w_down))
        contrib = from_experts(contrib)
        prob_back = from_experts(prob_back)
        picked = jnp.take_along_axis(contrib, target[:, :, None], axis=1)
        token_part = jnp.sum(picked.astype(jnp.float32).reshape(N_EXPERT, TOK_DEV, TOP, D), axis=2).astype(jnp.bfloat16)
        prob_part = jnp.take_along_axis(prob_back, target, axis=1).reshape(N_EXPERT, TOK_DEV, TOP)
        carry = tuple(total + part for total, part in zip(carry, grads))
        return carry, (token_part, prob_part)

    groups = (tokens.reshape(N_DP, N_EXPERT, TOK_DEV, D), out_grad.reshape(N_DP, N_EXPERT, TOK_DEV, D),
              expert_ids.reshape(N_DP, N_EXPERT, TOK_DEV, TOP), probs.reshape(N_DP, N_EXPERT, TOK_DEV, TOP))
    empty = jnp.zeros((EXPERTS, D, FF), jnp.float32)
    totals, outputs = lax.scan(group_pass, (empty, empty, empty), groups)
    token_grad = outputs[0].reshape(TOKENS, D)
    prob_grad = outputs[1].reshape(TOKENS, TOP)
    return token_grad, prob_grad, totals[0], totals[1], totals[2]
```

```python
import jax
import jax.numpy as jnp
from jax import lax
from jax.experimental import pallas as pl
from jax.experimental.pallas import tpu as pltpu
from jax.sharding import PartitionSpec as P

MESH = pl.DeviceIdType.MESH
F32, BF16 = jnp.float32, jnp.bfloat16
N = 8
OFF = (0, 1, 7, 2, 6, 3, 5, 4)
TOK, SLOT, D, FF, EXTRA = 16, 4, 2048, 384, 128
ROWS = N * N * SLOT
HALF = D // 2
GROUPS = 2
PER = N // GROUPS


def dot(a, b, ca=1, cb=0):
    return lax.dot_general(a, b, (((ca,), (cb,)), ((), ())), preferred_element_type=F32)


def iota(shape, axis):
    return lax.broadcasted_iota(jnp.int32, shape, axis)


def offset_of(k):
    return jnp.where(k % 2 == 1, (k + 1) // 2, (N - k // 2) % N)


def codes(weights):
    n = weights.shape[0]
    mask = weights.astype(F32) > 0.0
    r, c = iota((n, n), 0), iota((n, n), 1)
    before = jnp.where((r // TOK == c // TOK) & (c < r), 1.0, 0.0).astype(BF16)
    place = dot(before, jnp.where(mask, 1.0, 0.0).astype(BF16))
    return jnp.where(mask, place + 1.0, 0.0).astype(BF16)


def expert_lane(side, z, y, k):
    if side == 0:
        return z * N + (y + offset_of(k)) % N
    return ((z + offset_of(k)) % N) * N + y


def kernel(
    tok, dy, ids, pr, wg_h, wu_h, wd_h,
    tg_out, pg_out, gg_out, ug_out, dg_out,
    gather, send2, recv2, wgu, wd, gu, dyr, gbub, gbub_b, pact,
    contrib, back, tpart, trecv, part, other, ring_s, ring_r, ring1_s, ring1_r,
    wsem, p1s, p1r, p2s, p2r, c1s, c1r, c2s, c2r, ds, dr, rs, rr,
):
    dp, ex = lax.axis_index("dp"), lax.axis_index("expert")
    x, core = dp // 2, dp % 2
    z, y = ex // N, ex % N

    def along(side, d):
        if side == 0:
            return (dp, ((z + d) % N) * N + y)
        return (dp, z * N + (y + d) % N)

    ahead = (((x + 1) % N) * 2 + core, ex)
    behind = (((x + N - 1) % N) * 2 + core, ex)
    partner = (x * 2 + 1 - core, ex)

    loads = [
        pltpu.make_async_copy(wg_h.at[0], wgu.at[:, pl.ds(0, FF)], wsem.at[0]),
        pltpu.make_async_copy(wu_h.at[0], wgu.at[:, pl.ds(FF, FF)], wsem.at[1]),
        pltpu.make_async_copy(wd_h.at[0], wd, wsem.at[2]),
    ]
    for load in loads:
        load.start()

    barrier = pltpu.get_barrier_semaphore()
    peers = [along(side, d) for d in range(1, N) for side in range(2)] + [ahead, behind, partner]
    for peer in peers:
        pl.semaphore_signal(barrier, inc=1, device_id=peer, device_id_type=MESH)

    lane16 = iota((TOK, EXTRA), 1)
    dense = jnp.zeros((TOK, EXTRA), F32)
    for k in range(ids.shape[1]):
        dense += jnp.where(lane16 == ids[:, k : k + 1], pr[:, k : k + 1].astype(F32), 0.0)
    dense = dense.astype(BF16)
    for side, src in ((0, tok), (1, dy)):
        gather[side, 0:TOK, 0:D] = src[...]
        gather[side, 0:TOK, D : D + EXTRA] = dense

    pl.semaphore_wait(barrier, len(peers))

    sends = []

    def remote(src, dst, ssem, rsem, device):
        return pltpu.make_async_remote_copy(
            src_ref=src, dst_ref=dst, send_sem=ssem, recv_sem=rsem, device_id=device, device_id_type=MESH
        )

    def start(copy):
        copy.start()
        sends.append(copy)
        return copy

    hop1 = [[None] * N, [None] * N]
    for k in range(1, N):
        for side in range(2):
            hop1[side][k] = start(
                remote(
                    gather.at[side, pl.ds(0, TOK)], gather.at[side, pl.ds(TOK * k, TOK)],
                    p1s.at[side, k - 1], p1r.at[side, k - 1], along(side, OFF[k]),
                )
            )

    width = (D + EXTRA, D)
    hop2 = []
    for g in range(GROUPS):
        n_tok, n_row = PER * TOK, N * PER * SLOT
        for side in range(2):
            for k in range(max(1, g * PER), (g + 1) * PER):
                hop1[side][k].wait_recv()
            rows_at = pl.ds(g * n_tok, n_tok)
            code = codes(gather[side, rows_at, D : D + EXTRA])
            r, c = iota((n_row, EXTRA), 0), iota((n_row, EXTRA), 1)
            pick = jnp.where(c == expert_lane(side, z, y, r // (PER * SLOT)), 1.0, 0.0).astype(BF16)
            found = dot(pick, code, 1, 1)
            r, c = iota((n_row, n_tok), 0), iota((n_row, n_tok), 1)
            hit = (found == (r % SLOT + 1).astype(F32)) & ((r // SLOT) % PER == c // TOK)
            sel = jnp.where(hit, 1.0, 0.0).astype(BF16)

            def choose(cols, side=side, sel=sel, rows_at=rows_at, g=g):
                rows = dot(sel, gather[side, rows_at, cols]).astype(BF16)
                m = PER * SLOT
                for k in range(N):
                    target = send2 if k else recv2
                    target[side, pl.ds(k * N * SLOT + g * m, m), cols] = rows[k * m : (k + 1) * m]

            def tile(n, carry, choose=choose):
                choose(pl.ds(pl.multiple_of(n * 256, 256), 256))
                return carry

            lax.fori_loop(0, D // 256, tile, 0)
            if side == 0:
                choose(pl.ds(D, EXTRA))
            m = PER * SLOT
            for k in range(N - 1, 0, -1):
                at = pl.ds(k * N * SLOT + g * m, m)
                cols = pl.ds(0, width[side])
                hop2.append(
                    start(
                        remote(
                            send2.at[side, at, cols], recv2.at[side, at, cols],
                            p2s.at[side, g, k - 1], p2r.at[side, g, k - 1], along(1 - side, OFF[k]),
                        )
                    )
                )

    r, c = iota((ROWS, EXTRA), 0), iota((ROWS, EXTRA), 1)
    t, q = iota((N * TOK, ROWS), 0), iota((N * TOK, ROWS), 1)
    gives = []
    for side in range(2):
        code = codes(gather[side, :, D : D + EXTRA])
        pick = jnp.where(c == expert_lane(side, z, y, r // (N * SLOT)), 1.0, 0.0).astype(BF16)
        found = dot(code, pick, 1, 1)
        hit = (found == (q % SLOT + 1).astype(F32)) & ((q // SLOT) % N == t // TOK)
        gives.append(jnp.where(hit, 1.0, 0.0).astype(BF16))
    r, c = iota((ROWS, ROWS), 0), iota((ROWS, ROWS), 1)
    swapped = ((r // SLOT) % N) * (N * SLOT) + (r // (N * SLOT)) * SLOT + r % SLOT
    swap = jnp.where(c == swapped, 1.0, 0.0).astype(BF16)

    for load in loads:
        load.wait()
    for copy in hop2:
        copy.wait_recv()

    def tile_gu(n, carry):
        cols = pl.ds(pl.multiple_of(n * 256, 256), 256)
        gu[:, cols] = dot(recv2[0, :, 0:D], wgu[:, cols])
        return carry

    lax.fori_loop(0, 2 * FF // 256, tile_gu, 0)

    def tile_swap(n, carry):
        cols = pl.ds(pl.multiple_of(n * 256, 256), 256)
        dyr[:, cols] = dot(swap, recv2[1, :, cols]).astype(BF16)
        return carry

    lax.fori_loop(0, D // 256, tile_swap, 0)
    gu[:, 2 * FF : 3 * FF] = dot(dyr[...], wd[...])

    chunk = 32

    def middle(n, carry):
        at = pl.ds(pl.multiple_of(n * chunk, chunk), chunk)
        lane = iota((chunk, EXTRA), 1)
        p = jnp.sum(jnp.where(lane == ex, recv2[0, at, D : D + EXTRA].astype(F32), 0.0), axis=1, keepdims=True)
        gate, up, dyw = gu[at, 0:FF], gu[at, FF : 2 * FF], gu[at, 2 * FF : 3 * FF]
        sigma = 1.0 / (1.0 + jnp.exp(-gate))
        silu = gate * sigma
        act = (silu * up).astype(BF16).astype(F32)
        prob_back = jnp.sum(act * dyw, axis=1, keepdims=True)
        contrib[0, at, HALF : HALF + EXTRA] = jnp.where(lane == ex, prob_back, 0.0).astype(BF16)
        act_grad = p * dyw
        gbub[at, 0:FF] = (act_grad * up * sigma * (1.0 + gate * (1.0 - sigma))).astype(BF16)
        gbub[at, FF : 2 * FF] = (act_grad * silu).astype(BF16)
        pact[at, :] = (p * act).astype(BF16)
        return carry

    lax.fori_loop(0, ROWS // chunk, middle, 0)
    gbub_b[...] = dot(swap, gbub[...]).astype(BF16)

    line = N * SLOT
    widths = (HALF + EXTRA, HALF)
    back1 = []
    for side in range(2):
        mine = gbub if side == 0 else gbub_b

        def tile_c(n, carry, side=side, mine=mine):
            cols = pl.ds(pl.multiple_of(n * 256, 256), 256)
            w_rows = pl.ds(pl.multiple_of(side * HALF + n * 256, 256), 256)
            contrib[side, :, cols] = dot(mine[...], wgu[w_rows, :], 1, 1).astype(BF16)
            return carry

        lax.fori_loop(0, HALF // 256, tile_c, 0)
        cols = pl.ds(0, widths[side])
        for k in range(N - 1, 0, -1):
            at = pl.ds(k * line, line)
            back1.append(
                start(
                    remote(
                        contrib.at[side, at, cols], back.at[side, at, cols],
                        c1s.at[side, k - 1], c1r.at[side, k - 1], along(1 - side, N - OFF[k]),
                    )
                )
            )
        back[side, 0:line, cols] = contrib[side, 0:line, cols]

    def shards_gu(n, carry):
        cols = pl.ds(pl.multiple_of(((x + n) % N) * 256, 256), 256)
        both = dot(recv2[0, :, cols], gbub[...], 0, 0).astype(BF16)
        for m in range(2):
            for h in range(2):
                part[m, h, n] = both[h * 128 : h * 128 + 128, m * FF : (m + 1) * FF]
        return carry

    def shards_d(n, carry):
        cols = pl.ds(pl.multiple_of(((x + n) % N) * 256, 256), 256)
        both = dot(dyr[:, cols], pact[...], 0, 0).astype(BF16)
        for h in range(2):
            part[2, h, n] = both[h * 128 : h * 128 + 128]
        return carry

    swap_core = []

    def to_partner(m):
        swap_core.append(start(remote(part.at[m, 1 - core], other.at[m], ds.at[m], dr.at[m], partner)))

    lax.fori_loop(0, N, shards_gu, 0)
    to_partner(0)
    to_partner(1)
    lax.fori_loop(0, N, shards_d, 0)
    to_partner(2)

    def chip(m, rel, rows=pl.ds(0, 128)):
        return part[m, core, rel, rows, :].astype(F32) + other[m, rel, rows, :].astype(F32)

    towards = (ahead, behind)
    halves = (pl.ds(0, 64), pl.ds(64, 64))
    ring = {}
    for m in range(3):
        swap_core[m].wait_recv()
        for w in range(2):
            ring1_s[w, m] = chip(m, 4, halves[w]).astype(BF16)
            ring[w, 0, m] = start(
                remote(ring1_s.at[w, m], ring1_r.at[w, m], rs.at[w, 0, m], rr.at[w, 0, m], towards[w])
            )

    def ring_step(step):
        for m in range(3):
            for w in range(2):
                rel = 4 - step if w == 0 else 4 + step
                ring[w, step - 1, m].wait_recv()
                if step == 1:
                    a, b = halves[w], halves[1 - w]
                    ring_s[w, 0, m, a, :] = (chip(m, rel, a) + ring1_r[w, m].astype(F32)).astype(BF16)
                    ring_s[w, 0, m, b, :] = chip(m, rel, b).astype(BF16)
                else:
                    ring_s[w, step - 1, m] = (chip(m, rel) + ring_r[w, step - 2, m].astype(F32)).astype(BF16)
                ring[w, step, m] = start(
                    remote(
                        ring_s.at[w, step - 1, m], ring_r.at[w, step - 1, m],
                        rs.at[w, step, m], rr.at[w, step, m], towards[w],
                    )
                )

    ring_step(1)

    for copy in back1:
        copy.wait_recv()
    back_2 = []
    for side in range(2):
        for n in range(HALF // 256 + (side == 0)):
            size = 256 if n < HALF // 256 else EXTRA
            cols = pl.ds(n * 256, size)
            tpart[side, :, cols] = dot(gives[side], back[side, :, cols]).astype(BF16)
        cols = pl.ds(0, widths[side])
        for k in range(N - 1, 0, -1):
            at = pl.ds(k * TOK, TOK)
            back_2.append(
                start(
                    remote(
                        tpart.at[side, at, cols], trecv.at[side, at, cols],
                        c2s.at[side, k - 1], c2r.at[side, k - 1], along(side, N - OFF[k]),
                    )
                )
            )
        trecv[side, 0:TOK, cols] = tpart[side, 0:TOK, cols]

    ring_step(2)
    ring_step(3)

    for copy in back_2:
        copy.wait_recv()
    for side in range(2):
        total = jnp.zeros((TOK, HALF), F32)
        for k in range(N):
            total += trecv[side, k * TOK : (k + 1) * TOK, 0:HALF].astype(F32)
        tg_out[:, side * HALF : (side + 1) * HALF] = total.astype(BF16)
    dense = jnp.zeros((TOK, EXTRA), F32)
    for k in range(N):
        dense += trecv[0, k * TOK : (k + 1) * TOK, HALF : HALF + EXTRA].astype(F32)
    for k in range(ids.shape[1]):
        one = jnp.sum(jnp.where(lane16 == ids[:, k : k + 1], dense, 0.0), axis=1, keepdims=True)
        pg_out[:, k : k + 1] = one.astype(BF16)

    for m, out in enumerate((gg_out, ug_out, dg_out)):
        ring[0, 3, m].wait_recv()
        ring[1, 3, m].wait_recv()
        out[0] = chip(m, 0) + ring_r[0, 2, m].astype(F32) + ring_r[1, 2, m].astype(F32)

    for copy in sends:
        copy.wait_send()


def body(tokens, out_grad, expert_ids, probs, w_gate, w_up, w_down):
    vmem = pl.BlockSpec(memory_space=pltpu.VMEM)
    hbm = pl.BlockSpec(memory_space=pl.ANY)
    grads = jax.ShapeDtypeStruct((1, 128, FF), F32)
    dma = pltpu.SemaphoreType.DMA
    return pl.pallas_call(
        kernel,
        out_shape=(
            jax.ShapeDtypeStruct(tokens.shape, BF16),
            jax.ShapeDtypeStruct(probs.shape, BF16),
            grads, grads, grads,
        ),
        in_specs=[vmem] * 4 + [hbm] * 3,
        out_specs=(vmem,) * 5,
        scratch_shapes=[
            pltpu.VMEM((2, N * TOK, D + EXTRA), BF16),
            pltpu.VMEM((2, ROWS, D + EXTRA), BF16),
            pltpu.VMEM((2, ROWS, D + EXTRA), BF16),
            pltpu.VMEM((D, 2 * FF), BF16),
            pltpu.VMEM((D, FF), BF16),
            pltpu.VMEM((ROWS, 3 * FF), F32),
            pltpu.VMEM((ROWS, D), BF16),
            pltpu.VMEM((ROWS, 2 * FF), BF16),
            pltpu.VMEM((ROWS, 2 * FF), BF16),
            pltpu.VMEM((ROWS, FF), BF16),
            pltpu.VMEM((2, ROWS, HALF + EXTRA), BF16),
            pltpu.VMEM((2, ROWS, HALF + EXTRA), BF16),
            pltpu.VMEM((2, N * TOK, HALF + EXTRA), BF16),
            pltpu.VMEM((2, N * TOK, HALF + EXTRA), BF16),
            pltpu.VMEM((3, 2, N, 128, FF), BF16),
            pltpu.VMEM((3, N, 128, FF), BF16),
            pltpu.VMEM((2, 3, 3, 128, FF), BF16),
            pltpu.VMEM((2, 3, 3, 128, FF), BF16),
            pltpu.VMEM((2, 3, 64, FF), BF16),
            pltpu.VMEM((2, 3, 64, FF), BF16),
            dma((3,)),
            dma((2, N - 1)), dma((2, N - 1)),
            dma((2, GROUPS, N - 1)), dma((2, GROUPS, N - 1)),
            dma((2, N - 1)), dma((2, N - 1)),
            dma((2, N - 1)), dma((2, N - 1)),
            dma((3,)), dma((3,)),
            dma((2, 4, 3)), dma((2, 4, 3)),
        ],
        compiler_params=pltpu.CompilerParams(collective_id=0, has_side_effects=True),
        name="expert_layer_backward",
    )(tokens, out_grad, expert_ids, probs, w_gate, w_up, w_down)


def solution(mesh):
    rows = P(("dp", "expert"), None)
    weights = P("expert", None, None)
    grads = P("expert", "dp", None)
    return jax.shard_map(
        body,
        mesh=mesh,
        in_specs=(rows, rows, rows, rows, weights, weights, weights),
        out_specs=(rows, rows, grads, grads, grads),
        check_vma=False,
    )
```

```python
import jax
import jax.numpy as jnp
from jax import lax
from jax.experimental import pallas as pl
from jax.experimental.pallas import tpu as pltpu
from jax.sharding import PartitionSpec as P

MESH = pl.DeviceIdType.MESH
F32, BF16 = jnp.float32, jnp.bfloat16
N = 8
OFF = (0, 1, 7, 2, 6, 3, 5, 4)
TOK, SLOT, D, FF, EXTRA = 16, 4, 2048, 384, 128
ROWS = N * N * SLOT
HALF = D // 2
GROUPS = 2
VMEM_LIMIT = 209 << 18
PER = N // GROUPS


def dot(a, b, ca=1, cb=0):
    return lax.dot_general(a, b, (((ca,), (cb,)), ((), ())), preferred_element_type=F32)


def iota(shape, axis):
    return lax.broadcasted_iota(jnp.int32, shape, axis)


def offset_of(k):
    return jnp.where(k % 2 == 1, (k + 1) // 2, (N - k // 2) % N)


def codes(weights):
    n = weights.shape[0]
    mask = weights.astype(F32) > 0.0
    r, c = iota((n, n), 0), iota((n, n), 1)
    before = jnp.where((r // TOK == c // TOK) & (c < r), 1.0, 0.0).astype(BF16)
    place = dot(before, jnp.where(mask, 1.0, 0.0).astype(BF16))
    return jnp.where(mask, place + 1.0, 0.0).astype(BF16)


def expert_lane(side, z, y, k):
    if side == 0:
        return z * N + (y + offset_of(k)) % N
    return ((z + offset_of(k)) % N) * N + y


def kernel(
    tok, dy, ids, pr, wg_h, wu_h, wd_h,
    tg_out, pg_out, grads_out,
    gather, send2, recv2, wgu, wd, gu, dyr, gbub, gbub_b, pact,
    contrib, back, tpart, trecv, part, other, ring_s, ring_r, ring1_s, ring1_r,
    wsem, p1s, p1r, p2s, p2r, c1s, c1r, c2s, c2r, ds, dr, rs, rr,
):
    dp, ex = lax.axis_index("dp"), lax.axis_index("expert")
    x, core = dp // 2, dp % 2
    z, y = ex // N, ex % N

    def along(side, d):
        if side == 0:
            return (dp, ((z + d) % N) * N + y)
        return (dp, z * N + (y + d) % N)

    ahead = (((x + 1) % N) * 2 + core, ex)
    behind = (((x + N - 1) % N) * 2 + core, ex)
    partner = (x * 2 + 1 - core, ex)

    loads = [
        pltpu.make_async_copy(wg_h.at[0], wgu.at[:, pl.ds(0, FF)], wsem.at[0]),
        pltpu.make_async_copy(wu_h.at[0], wgu.at[:, pl.ds(FF, FF)], wsem.at[1]),
        pltpu.make_async_copy(wd_h.at[0], wd, wsem.at[2]),
    ]
    for load in loads:
        load.start()

    barrier = pltpu.get_barrier_semaphore()
    peers = [along(side, d) for d in range(1, N) for side in range(2)] + [ahead, behind, partner]
    for peer in peers:
        pl.semaphore_signal(barrier, inc=1, device_id=peer, device_id_type=MESH)

    top = ids.shape[0]
    wide = pr[...].astype(F32)
    expert = iota((EXTRA, TOK), 0)
    dense = jnp.zeros((EXTRA, TOK), F32)
    for k in range(top):
        dense += jnp.where(expert == ids[k : k + 1, :], wide[k : k + 1, :], 0.0)
    dense = dense.T.astype(BF16)
    for side, src in ((0, tok), (1, dy)):
        gather[side, 0:TOK, 0:D] = src[...]
        gather[side, 0:TOK, D : D + EXTRA] = dense

    pl.semaphore_wait(barrier, len(peers))

    sends = []

    def remote(src, dst, ssem, rsem, device):
        return pltpu.make_async_remote_copy(
            src_ref=src, dst_ref=dst, send_sem=ssem, recv_sem=rsem, device_id=device, device_id_type=MESH
        )

    def start(copy):
        copy.start()
        sends.append(copy)
        return copy

    def share(side, i, src_slab, dst_slab, d, cols):
        src, dst = (gather.at[side, pl.ds(TOK * k, TOK), cols] for k in (src_slab, dst_slab))
        return start(remote(src, dst, p1s.at[side, i], p1r.at[side, i], along(side, d % N)))

    every = pl.ds(0, D + EXTRA)
    first, second = pl.ds(0, HALF), pl.ds(HALF, HALF + EXTRA)
    hop1 = [[[] for _ in range(N)] for _ in range(2)]
    for k in (3, 4, 1, 2):
        for side in range(2):
            hop1[side][k].append(share(side, k - 1, 0, k, OFF[k], every))
    for slab, to, d, i, cols in ((3, 5, 1, 6, first), (4, 6, -1, 7, second)):
        for side in range(2):
            for copy in hop1[side][slab]:
                copy.wait_recv()
            hop1[side][slab] = []
            hop1[side][to].append(share(side, to - 1, slab, to, d, every))
            hop1[side][N - 1].append(share(side, i, slab, N - 1, 2 * d, cols))

    width = (D + EXTRA, D)
    hop2 = []
    for g in range(GROUPS):
        n_tok, n_row = PER * TOK, N * PER * SLOT
        for side in range(2):
            for k in range(g * PER, (g + 1) * PER):
                for copy in hop1[side][k]:
                    copy.wait_recv()
            rows_at = pl.ds(g * n_tok, n_tok)
            code = codes(gather[side, rows_at, D : D + EXTRA])
            r, c = iota((n_row, EXTRA), 0), iota((n_row, EXTRA), 1)
            pick = jnp.where(c == expert_lane(side, z, y, r // (PER * SLOT)), 1.0, 0.0).astype(BF16)
            found = dot(pick, code, 1, 1)
            r, c = iota((n_row, n_tok), 0), iota((n_row, n_tok), 1)
            hit = (found == (r % SLOT + 1).astype(F32)) & ((r // SLOT) % PER == c // TOK)
            sel = jnp.where(hit, 1.0, 0.0).astype(BF16)

            def choose(cols, side=side, sel=sel, rows_at=rows_at, g=g):
                rows = dot(sel, gather[side, rows_at, cols]).astype(BF16)
                m = PER * SLOT
                for k in range(N):
                    target = send2 if k else recv2
                    target[side, pl.ds(k * N * SLOT + g * m, m), cols] = rows[k * m : (k + 1) * m]

            def tile(n, carry, choose=choose):
                choose(pl.ds(pl.multiple_of(n * 256, 256), 256))
                return carry

            lax.fori_loop(0, D // 256, tile, 0)
            if side == 0:
                choose(pl.ds(D, EXTRA))
            m = PER * SLOT
            for k in range(N - 1, 0, -1):
                at = pl.ds(k * N * SLOT + g * m, m)
                cols = pl.ds(0, width[side])
                hop2.append(
                    start(
                        remote(
                            send2.at[side, at, cols], recv2.at[side, at, cols],
                            p2s.at[side, g, k - 1], p2r.at[side, g, k - 1], along(1 - side, OFF[k]),
                        )
                    )
                )

    r, c = iota((ROWS, EXTRA), 0), iota((ROWS, EXTRA), 1)
    t, q = iota((N * TOK, ROWS), 0), iota((N * TOK, ROWS), 1)
    gives = []
    for side in range(2):
        code = codes(gather[side, :, D : D + EXTRA])
        pick = jnp.where(c == expert_lane(side, z, y, r // (N * SLOT)), 1.0, 0.0).astype(BF16)
        found = dot(code, pick, 1, 1)
        hit = (found == (q % SLOT + 1).astype(F32)) & ((q // SLOT) % N == t // TOK)
        gives.append(jnp.where(hit, 1.0, 0.0).astype(BF16))
    r, c = iota((ROWS, ROWS), 0), iota((ROWS, ROWS), 1)
    swapped = ((r // SLOT) % N) * (N * SLOT) + (r // (N * SLOT)) * SLOT + r % SLOT
    swap = jnp.where(c == swapped, 1.0, 0.0).astype(BF16)

    for load in loads:
        load.wait()
    for copy in hop2:
        copy.wait_recv()

    def tile_gu(n, carry):
        cols = pl.ds(pl.multiple_of(n * 256, 256), 256)
        gu[:, cols] = dot(recv2[0, :, 0:D], wgu[:, cols])
        return carry

    lax.fori_loop(0, 2 * FF // 256, tile_gu, 0)

    def tile_swap(n, carry):
        cols = pl.ds(pl.multiple_of(n * 256, 256), 256)
        dyr[:, cols] = dot(swap, recv2[1, :, cols]).astype(BF16)
        return carry

    lax.fori_loop(0, D // 256, tile_swap, 0)
    gu[:, 2 * FF : 3 * FF] = dot(dyr[...], wd[...])

    chunk = 32

    def middle(n, carry):
        at = pl.ds(pl.multiple_of(n * chunk, chunk), chunk)
        lane = iota((chunk, EXTRA), 1)
        p = jnp.sum(jnp.where(lane == ex, recv2[0, at, D : D + EXTRA].astype(F32), 0.0), axis=1, keepdims=True)
        gate, up, dyw = gu[at, 0:FF], gu[at, FF : 2 * FF], gu[at, 2 * FF : 3 * FF]
        sigma = 1.0 / (1.0 + jnp.exp(-gate))
        silu = gate * sigma
        act = (silu * up).astype(BF16).astype(F32)
        prob_back = jnp.sum(act * dyw, axis=1, keepdims=True)
        contrib[0, at, HALF : HALF + EXTRA] = jnp.where(lane == ex, prob_back, 0.0).astype(BF16)
        act_grad = p * dyw
        gbub[at, 0:FF] = (act_grad * up * sigma * (1.0 + gate * (1.0 - sigma))).astype(BF16)
        gbub[at, FF : 2 * FF] = (act_grad * silu).astype(BF16)
        pact[at, :] = (p * act).astype(BF16)
        return carry

    lax.fori_loop(0, ROWS // chunk, middle, 0)
    gbub_b[...] = dot(swap, gbub[...]).astype(BF16)

    swap_core = {}

    def shards(n):
        cols = pl.ds(pl.multiple_of(((x + n) % N) * 256, 256), 256)
        both = dot(recv2[0, :, cols], gbub[...], 0, 0).astype(BF16)
        down = dot(dyr[:, cols], pact[...], 0, 0).astype(BF16)
        for h in range(2):
            rows = slice(h * 128, h * 128 + 128)
            part[n, h, 0] = both[rows, 0:FF]
            part[n, h, 1] = both[rows, FF : 2 * FF]
            part[n, h, 2] = down[rows]
        swap_core[n] = start(remote(part.at[n, 1 - core], other.at[n], ds.at[n], dr.at[n], partner))

    def chip(m, rel, rows=pl.ds(0, 128)):
        return part[rel, core, m, rows, :].astype(F32) + other[rel, m, rows, :].astype(F32)

    for n in (4, 3, 5):
        shards(n)

    towards = (ahead, behind)
    halves = (pl.ds(0, 64), pl.ds(64, 64))
    ring = {}
    swap_core[4].wait_recv()
    for m in range(3):
        for w in range(2):
            ring1_s[w, m] = chip(m, 4, halves[w]).astype(BF16)
            ring[w, 0, m] = start(
                remote(ring1_s.at[w, m], ring1_r.at[w, m], rs.at[w, 0, m], rr.at[w, 0, m], towards[w])
            )

    for n in (2, 6, 1, 7, 0):
        shards(n)

    line = N * SLOT
    widths = (HALF + EXTRA, HALF)
    back1 = []
    for side in range(2):
        mine = gbub if side == 0 else gbub_b

        def tile_c(n, carry, side=side, mine=mine):
            cols = pl.ds(pl.multiple_of(n * 256, 256), 256)
            w_rows = pl.ds(pl.multiple_of(side * HALF + n * 256, 256), 256)
            contrib[side, :, cols] = dot(mine[...], wgu[w_rows, :], 1, 1).astype(BF16)
            return carry

        lax.fori_loop(0, HALF // 256, tile_c, 0)
        cols = pl.ds(0, widths[side])
        for k in range(N - 1, 0, -1):
            at = pl.ds(k * line, line)
            back1.append(
                start(
                    remote(
                        contrib.at[side, at, cols], back.at[side, at, cols],
                        c1s.at[side, k - 1], c1r.at[side, k - 1], along(1 - side, N - OFF[k]),
                    )
                )
            )
        back[side, 0:line, cols] = contrib[side, 0:line, cols]

    def ring_step(step):
        swap_core[4 - step].wait_recv()
        swap_core[4 + step].wait_recv()
        for m in range(3):
            for w in range(2):
                rel = 4 - step if w == 0 else 4 + step
                ring[w, step - 1, m].wait_recv()
                if step == 1:
                    a, b = halves[w], halves[1 - w]
                    ring_s[w, 0, m, a, :] = (chip(m, rel, a) + ring1_r[w, m].astype(F32)).astype(BF16)
                    ring_s[w, 0, m, b, :] = chip(m, rel, b).astype(BF16)
                else:
                    ring_s[w, step - 1, m] = (chip(m, rel) + ring_r[w, step - 2, m].astype(F32)).astype(BF16)
                ring[w, step, m] = start(
                    remote(
                        ring_s.at[w, step - 1, m], ring_r.at[w, step - 1, m],
                        rs.at[w, step, m], rr.at[w, step, m], towards[w],
                    )
                )

    ring_step(1)
    ring_step(2)

    for copy in back1:
        copy.wait_recv()
    back_2 = []
    for side in range(2):
        for n in range(HALF // 256 + (side == 0)):
            size = 256 if n < HALF // 256 else EXTRA
            cols = pl.ds(n * 256, size)
            tpart[side, :, cols] = dot(gives[side], back[side, :, cols]).astype(BF16)
        cols = pl.ds(0, widths[side])
        for k in range(N - 1, 0, -1):
            at = pl.ds(k * TOK, TOK)
            back_2.append(
                start(
                    remote(
                        tpart.at[side, at, cols], trecv.at[side, at, cols],
                        c2s.at[side, k - 1], c2r.at[side, k - 1], along(side, N - OFF[k]),
                    )
                )
            )
        trecv[side, 0:TOK, cols] = tpart[side, 0:TOK, cols]

    ring_step(3)

    for copy in back_2:
        copy.wait_recv()
    for side in range(2):
        total = jnp.zeros((TOK, HALF), F32)
        for k in range(N):
            total += trecv[side, k * TOK : (k + 1) * TOK, 0:HALF].astype(F32)
        tg_out[:, side * HALF : (side + 1) * HALF] = total.astype(BF16)
    dense = jnp.zeros((TOK, EXTRA), F32)
    for k in range(N):
        dense += trecv[0, k * TOK : (k + 1) * TOK, HALF : HALF + EXTRA].astype(F32)
    dense = dense.T
    for k in range(top):
        one = jnp.where(expert == ids[k : k + 1, :], dense, 0.0)
        pg_out[k : k + 1, :] = jnp.sum(one, axis=0, keepdims=True)

    swap_core[0].wait_recv()
    for m in range(3):
        ring[0, 3, m].wait_recv()
        ring[1, 3, m].wait_recv()
        grads_out[m] = chip(m, 0) + ring_r[0, 2, m].astype(F32) + ring_r[1, 2, m].astype(F32)

    for copy in sends:
        copy.wait_send()


def finish(tg, pg, grads, tg_out, pg_out, gg_out, ug_out, dg_out):
    tg_out[...] = tg[...]
    pg_out[...] = pg[...].astype(BF16)
    for m, out in enumerate((gg_out, ug_out, dg_out)):
        out[0] = grads[m]


def body(tokens, out_grad, expert_ids, probs, w_gate, w_up, w_down):
    vmem = pl.BlockSpec(memory_space=pltpu.VMEM)
    hbm = pl.BlockSpec(memory_space=pltpu.HBM)
    grads = jax.ShapeDtypeStruct((1, 128, FF), F32)
    token_grad = jax.ShapeDtypeStruct(tokens.shape, BF16)
    small = probs.T.shape
    dma = pltpu.SemaphoreType.DMA
    sums = pl.pallas_call(
        kernel,
        out_shape=(token_grad, jax.ShapeDtypeStruct(small, F32), jax.ShapeDtypeStruct((3, 128, FF), F32)),
        in_specs=[vmem] * 4 + [hbm] * 3,
        out_specs=(vmem,) * 3,
        scratch_shapes=[
            pltpu.VMEM((2, N * TOK, D + EXTRA), BF16),
            pltpu.VMEM((2, ROWS, D + EXTRA), BF16),
            pltpu.VMEM((2, ROWS, D + EXTRA), BF16),
            pltpu.VMEM((D, 2 * FF), BF16),
            pltpu.VMEM((D, FF), BF16),
            pltpu.VMEM((ROWS, 3 * FF), F32),
            pltpu.VMEM((ROWS, D), BF16),
            pltpu.VMEM((ROWS, 2 * FF), BF16),
            pltpu.VMEM((ROWS, 2 * FF), BF16),
            pltpu.VMEM((ROWS, FF), BF16),
            pltpu.VMEM((2, ROWS, HALF + EXTRA), BF16),
            pltpu.VMEM((2, ROWS, HALF + EXTRA), BF16),
            pltpu.VMEM((2, N * TOK, HALF + EXTRA), BF16),
            pltpu.VMEM((2, N * TOK, HALF + EXTRA), BF16),
            pltpu.VMEM((N, 2, 3, 128, FF), BF16),
            pltpu.VMEM((N, 3, 128, FF), BF16),
            pltpu.VMEM((2, 3, 3, 128, FF), BF16),
            pltpu.VMEM((2, 3, 3, 128, FF), BF16),
            pltpu.VMEM((2, 3, 64, FF), BF16),
            pltpu.VMEM((2, 3, 64, FF), BF16),
            dma((3,)),
            dma((2, N)), dma((2, N)),
            dma((2, GROUPS, N - 1)), dma((2, GROUPS, N - 1)),
            dma((2, N - 1)), dma((2, N - 1)),
            dma((2, N - 1)), dma((2, N - 1)),
            dma((N,)), dma((N,)),
            dma((2, 4, 3)), dma((2, 4, 3)),
        ],
        compiler_params=pltpu.CompilerParams(collective_id=0, has_side_effects=True, vmem_limit_bytes=VMEM_LIMIT),
        name="expert_layer_backward",
    )(tokens, out_grad, expert_ids.T, probs.T, w_gate, w_up, w_down)
    token_grad, prob_grad, *weight_grads = pl.pallas_call(
        finish,
        out_shape=(token_grad, jax.ShapeDtypeStruct(small, BF16), grads, grads, grads),
        in_specs=[vmem] * 3,
        out_specs=(vmem,) * 5,
        compiler_params=pltpu.CompilerParams(vmem_limit_bytes=4 << 20),
        name="write_outputs",
    )(*sums)
    return (token_grad, prob_grad.T, *weight_grads)


def solution(mesh):
    rows = P(("dp", "expert"), None)
    weights = P("expert", None, None)
    grads = P("expert", "dp", None)
    return jax.shard_map(
        body,
        mesh=mesh,
        in_specs=(rows, rows, rows, rows, weights, weights, weights),
        out_specs=(rows, rows, grads, grads, grads),
        check_vma=False,
    )
```

```python
import jax
import jax.numpy as jnp
from jax import lax
from jax.experimental import pallas as pl
from jax.experimental.pallas import tpu as pltpu
from jax.sharding import PartitionSpec as P

MESH = pl.DeviceIdType.MESH
F32, BF16 = jnp.float32, jnp.bfloat16
N = 8
OFF = (0, 1, 7, 2, 6, 3, 5, 4)
TOK, SLOT, D, FF, EXTRA = 16, 4, 2048, 384, 128
ROWS = N * N * SLOT
HALF = D // 2
GROUPS = 2
VMEM_LIMIT = 209 << 18
PER = N // GROUPS


def dot(a, b, ca=1, cb=0):
    return lax.dot_general(a, b, (((ca,), (cb,)), ((), ())), preferred_element_type=F32)


def iota(shape, axis):
    return lax.broadcasted_iota(jnp.int32, shape, axis)


def offset_of(k):
    return jnp.where(k % 2 == 1, (k + 1) // 2, (N - k // 2) % N)


def codes(weights):
    n = weights.shape[0]
    mask = weights.astype(F32) > 0.0
    r, c = iota((n, n), 0), iota((n, n), 1)
    before = jnp.where((r // TOK == c // TOK) & (c < r), 1.0, 0.0).astype(BF16)
    place = dot(before, jnp.where(mask, 1.0, 0.0).astype(BF16))
    return jnp.where(mask, place + 1.0, 0.0).astype(BF16)


def expert_lane(side, z, y, k):
    if side == 0:
        return z * N + (y + offset_of(k)) % N
    return ((z + offset_of(k)) % N) * N + y


def kernel(
    tok_h, dy_h, ids_h, pr_h, wg_h, wu_h, wd_h,
    tg_out, pg_out, grads_out,
    ids, pr, gather, send2, recv2, wgu, wd, gu, dyr, gbub, gbub_b, pact,
    contrib, back, tpart, trecv, part, other, ring_s, ring_r, ring1_s, ring1_r,
    isem, wsem, p1s, p1r, p2s, p2r, c1s, c1r, c2s, c2r, ds, dr, rs, rr,
):
    dp, ex = lax.axis_index("dp"), lax.axis_index("expert")
    x, core = dp // 2, dp % 2
    z, y = ex // N, ex % N

    def along(side, d):
        if side == 0:
            return (dp, ((z + d) % N) * N + y)
        return (dp, z * N + (y + d) % N)

    ahead = (((x + 1) % N) * 2 + core, ex)
    behind = (((x + N - 1) % N) * 2 + core, ex)
    partner = (x * 2 + 1 - core, ex)

    inputs = [
        pltpu.make_async_copy(src, dst, isem.at[i])
        for i, (src, dst) in enumerate((
            (ids_h, ids), (pr_h, pr),
            (tok_h, gather.at[0, pl.ds(0, TOK), pl.ds(0, D)]), (dy_h, gather.at[1, pl.ds(0, TOK), pl.ds(0, D)]),
        ))
    ]
    for load in inputs:
        load.start()
    loads = [
        pltpu.make_async_copy(wg_h.at[0], wgu.at[:, pl.ds(0, FF)], wsem.at[0]),
        pltpu.make_async_copy(wu_h.at[0], wgu.at[:, pl.ds(FF, FF)], wsem.at[1]),
        pltpu.make_async_copy(wd_h.at[0], wd, wsem.at[2]),
    ]
    for load in loads:
        load.start()

    barrier = pltpu.get_barrier_semaphore()
    peers = [along(side, d) for d in range(1, N) for side in range(2)] + [ahead, behind, partner]
    for peer in peers:
        pl.semaphore_signal(barrier, inc=1, device_id=peer, device_id_type=MESH)

    for load in inputs:
        load.wait()
    top = ids.shape[0]
    wide = pr[...].astype(F32)
    expert = iota((EXTRA, TOK), 0)
    dense = jnp.zeros((EXTRA, TOK), F32)
    for k in range(top):
        dense += jnp.where(expert == ids[k : k + 1, :], wide[k : k + 1, :], 0.0)
    dense = dense.T.astype(BF16)
    for side in range(2):
        gather[side, 0:TOK, D : D + EXTRA] = dense

    pl.semaphore_wait(barrier, len(peers))

    sends = []

    def remote(src, dst, ssem, rsem, device):
        return pltpu.make_async_remote_copy(
            src_ref=src, dst_ref=dst, send_sem=ssem, recv_sem=rsem, device_id=device, device_id_type=MESH
        )

    def start(copy):
        copy.start()
        sends.append(copy)
        return copy

    def share(side, i, src_slab, dst_slab, d, cols):
        src, dst = (gather.at[side, pl.ds(TOK * k, TOK), cols] for k in (src_slab, dst_slab))
        return start(remote(src, dst, p1s.at[side, i], p1r.at[side, i], along(side, d % N)))

    every = pl.ds(0, D + EXTRA)
    first, second = pl.ds(0, HALF), pl.ds(HALF, HALF + EXTRA)
    hop1 = [[[] for _ in range(N)] for _ in range(2)]
    for k in (3, 4, 1, 2):
        for side in range(2):
            hop1[side][k].append(share(side, k - 1, 0, k, OFF[k], every))
    for slab, to, d, i, cols in ((3, 5, 1, 6, first), (4, 6, -1, 7, second)):
        for side in range(2):
            for copy in hop1[side][slab]:
                copy.wait_recv()
            hop1[side][slab] = []
            hop1[side][to].append(share(side, to - 1, slab, to, d, every))
            hop1[side][N - 1].append(share(side, i, slab, N - 1, 2 * d, cols))

    width = (D + EXTRA, D)
    hop2 = []
    for g in range(GROUPS):
        n_tok, n_row = PER * TOK, N * PER * SLOT
        for side in range(2):
            for k in range(g * PER, (g + 1) * PER):
                for copy in hop1[side][k]:
                    copy.wait_recv()
            rows_at = pl.ds(g * n_tok, n_tok)
            code = codes(gather[side, rows_at, D : D + EXTRA])
            r, c = iota((n_row, EXTRA), 0), iota((n_row, EXTRA), 1)
            pick = jnp.where(c == expert_lane(side, z, y, r // (PER * SLOT)), 1.0, 0.0).astype(BF16)
            found = dot(pick, code, 1, 1)
            r, c = iota((n_row, n_tok), 0), iota((n_row, n_tok), 1)
            hit = (found == (r % SLOT + 1).astype(F32)) & ((r // SLOT) % PER == c // TOK)
            sel = jnp.where(hit, 1.0, 0.0).astype(BF16)

            def choose(cols, side=side, sel=sel, rows_at=rows_at, g=g):
                rows = dot(sel, gather[side, rows_at, cols]).astype(BF16)
                m = PER * SLOT
                for k in range(N):
                    target = send2 if k else recv2
                    target[side, pl.ds(k * N * SLOT + g * m, m), cols] = rows[k * m : (k + 1) * m]

            def tile(n, carry, choose=choose):
                choose(pl.ds(pl.multiple_of(n * 256, 256), 256))
                return carry

            lax.fori_loop(0, D // 256, tile, 0)
            if side == 0:
                choose(pl.ds(D, EXTRA))
            m = PER * SLOT
            for k in range(N - 1, 0, -1):
                at = pl.ds(k * N * SLOT + g * m, m)
                cols = pl.ds(0, width[side])
                hop2.append(
                    start(
                        remote(
                            send2.at[side, at, cols], recv2.at[side, at, cols],
                            p2s.at[side, g, k - 1], p2r.at[side, g, k - 1], along(1 - side, OFF[k]),
                        )
                    )
                )

    r, c = iota((ROWS, EXTRA), 0), iota((ROWS, EXTRA), 1)
    t, q = iota((N * TOK, ROWS), 0), iota((N * TOK, ROWS), 1)
    gives = []
    for side in range(2):
        code = codes(gather[side, :, D : D + EXTRA])
        pick = jnp.where(c == expert_lane(side, z, y, r // (N * SLOT)), 1.0, 0.0).astype(BF16)
        found = dot(code, pick, 1, 1)
        hit = (found == (q % SLOT + 1).astype(F32)) & ((q // SLOT) % N == t // TOK)
        gives.append(jnp.where(hit, 1.0, 0.0).astype(BF16))
    r, c = iota((ROWS, ROWS), 0), iota((ROWS, ROWS), 1)
    swapped = ((r // SLOT) % N) * (N * SLOT) + (r // (N * SLOT)) * SLOT + r % SLOT
    swap = jnp.where(c == swapped, 1.0, 0.0).astype(BF16)

    for load in loads:
        load.wait()
    for copy in hop2:
        copy.wait_recv()

    def tile_gu(n, carry):
        cols = pl.ds(pl.multiple_of(n * 256, 256), 256)
        gu[:, cols] = dot(recv2[0, :, 0:D], wgu[:, cols])
        return carry

    lax.fori_loop(0, 2 * FF // 256, tile_gu, 0)

    def tile_swap(n, carry):
        cols = pl.ds(pl.multiple_of(n * 256, 256), 256)
        dyr[:, cols] = dot(swap, recv2[1, :, cols]).astype(BF16)
        return carry

    lax.fori_loop(0, D // 256, tile_swap, 0)
    gu[:, 2 * FF : 3 * FF] = dot(dyr[...], wd[...])

    chunk = 32

    def middle(n, carry):
        at = pl.ds(pl.multiple_of(n * chunk, chunk), chunk)
        lane = iota((chunk, EXTRA), 1)
        p = jnp.sum(jnp.where(lane == ex, recv2[0, at, D : D + EXTRA].astype(F32), 0.0), axis=1, keepdims=True)
        gate, up, dyw = gu[at, 0:FF], gu[at, FF : 2 * FF], gu[at, 2 * FF : 3 * FF]
        sigma = 1.0 / (1.0 + jnp.exp(-gate))
        silu = gate * sigma
        act = (silu * up).astype(BF16).astype(F32)
        prob_back = jnp.sum(act * dyw, axis=1, keepdims=True)
        contrib[0, at, HALF : HALF + EXTRA] = jnp.where(lane == ex, prob_back, 0.0).astype(BF16)
        act_grad = p * dyw
        gbub[at, 0:FF] = (act_grad * up * sigma * (1.0 + gate * (1.0 - sigma))).astype(BF16)
        gbub[at, FF : 2 * FF] = (act_grad * silu).astype(BF16)
        pact[at, :] = (p * act).astype(BF16)
        return carry

    lax.fori_loop(0, ROWS // chunk, middle, 0)
    gbub_b[...] = dot(swap, gbub[...]).astype(BF16)

    swap_core = {}

    def shards(n):
        cols = pl.ds(pl.multiple_of(((x + n) % N) * 256, 256), 256)
        both = dot(recv2[0, :, cols], gbub[...], 0, 0).astype(BF16)
        down = dot(dyr[:, cols], pact[...], 0, 0).astype(BF16)
        for h in range(2):
            rows = slice(h * 128, h * 128 + 128)
            part[n, h, 0] = both[rows, 0:FF]
            part[n, h, 1] = both[rows, FF : 2 * FF]
            part[n, h, 2] = down[rows]
        swap_core[n] = start(remote(part.at[n, 1 - core], other.at[n], ds.at[n], dr.at[n], partner))

    def chip(m, rel, rows=pl.ds(0, 128)):
        return part[rel, core, m, rows, :].astype(F32) + other[rel, m, rows, :].astype(F32)

    for n in (4, 3, 5):
        shards(n)

    towards = (ahead, behind)
    halves = (pl.ds(0, 64), pl.ds(64, 64))
    ring = {}
    swap_core[4].wait_recv()
    for m in range(3):
        for w in range(2):
            ring1_s[w, m] = chip(m, 4, halves[w]).astype(BF16)
            ring[w, 0, m] = start(
                remote(ring1_s.at[w, m], ring1_r.at[w, m], rs.at[w, 0, m], rr.at[w, 0, m], towards[w])
            )

    for n in (2, 6, 1, 7, 0):
        shards(n)

    line = N * SLOT
    widths = (HALF + EXTRA, HALF)
    back1 = []
    for side in range(2):
        mine = gbub if side == 0 else gbub_b

        def tile_c(n, carry, side=side, mine=mine):
            cols = pl.ds(pl.multiple_of(n * 256, 256), 256)
            w_rows = pl.ds(pl.multiple_of(side * HALF + n * 256, 256), 256)
            contrib[side, :, cols] = dot(mine[...], wgu[w_rows, :], 1, 1).astype(BF16)
            return carry

        lax.fori_loop(0, HALF // 256, tile_c, 0)
        cols = pl.ds(0, widths[side])
        for k in range(N - 1, 0, -1):
            at = pl.ds(k * line, line)
            back1.append(
                start(
                    remote(
                        contrib.at[side, at, cols], back.at[side, at, cols],
                        c1s.at[side, k - 1], c1r.at[side, k - 1], along(1 - side, N - OFF[k]),
                    )
                )
            )
        back[side, 0:line, cols] = contrib[side, 0:line, cols]

    def ring_step(step):
        swap_core[4 - step].wait_recv()
        swap_core[4 + step].wait_recv()
        for m in range(3):
            for w in range(2):
                rel = 4 - step if w == 0 else 4 + step
                ring[w, step - 1, m].wait_recv()
                if step == 1:
                    a, b = halves[w], halves[1 - w]
                    ring_s[w, 0, m, a, :] = (chip(m, rel, a) + ring1_r[w, m].astype(F32)).astype(BF16)
                    ring_s[w, 0, m, b, :] = chip(m, rel, b).astype(BF16)
                else:
                    ring_s[w, step - 1, m] = (chip(m, rel) + ring_r[w, step - 2, m].astype(F32)).astype(BF16)
                ring[w, step, m] = start(
                    remote(
                        ring_s.at[w, step - 1, m], ring_r.at[w, step - 1, m],
                        rs.at[w, step, m], rr.at[w, step, m], towards[w],
                    )
                )

    ring_step(1)
    ring_step(2)

    for copy in back1:
        copy.wait_recv()
    back_2 = []
    for side in range(2):
        for n in range(HALF // 256 + (side == 0)):
            size = 256 if n < HALF // 256 else EXTRA
            cols = pl.ds(n * 256, size)
            tpart[side, :, cols] = dot(gives[side], back[side, :, cols]).astype(BF16)
        cols = pl.ds(0, widths[side])
        for k in range(N - 1, 0, -1):
            at = pl.ds(k * TOK, TOK)
            back_2.append(
                start(
                    remote(
                        tpart.at[side, at, cols], trecv.at[side, at, cols],
                        c2s.at[side, k - 1], c2r.at[side, k - 1], along(side, N - OFF[k]),
                    )
                )
            )
        trecv[side, 0:TOK, cols] = tpart[side, 0:TOK, cols]

    ring_step(3)

    for copy in back_2:
        copy.wait_recv()
    for side in range(2):
        total = jnp.zeros((TOK, HALF), F32)
        for k in range(N):
            total += trecv[side, k * TOK : (k + 1) * TOK, 0:HALF].astype(F32)
        tg_out[:, side * HALF : (side + 1) * HALF] = total.astype(BF16)
    dense = jnp.zeros((TOK, EXTRA), F32)
    for k in range(N):
        dense += trecv[0, k * TOK : (k + 1) * TOK, HALF : HALF + EXTRA].astype(F32)
    dense = dense.T
    for k in range(top):
        one = jnp.where(expert == ids[k : k + 1, :], dense, 0.0)
        pg_out[k : k + 1, :] = jnp.sum(one, axis=0, keepdims=True)

    swap_core[0].wait_recv()
    for m in range(3):
        ring[0, 3, m].wait_recv()
        ring[1, 3, m].wait_recv()
        grads_out[m] = chip(m, 0) + ring_r[0, 2, m].astype(F32) + ring_r[1, 2, m].astype(F32)

    for copy in sends:
        copy.wait_send()


def finish(tg, pg, grads, tg_out, pg_out, gg_out, ug_out, dg_out):
    tg_out[...] = tg[...]
    pg_out[...] = pg[...].astype(BF16)
    for m, out in enumerate((gg_out, ug_out, dg_out)):
        out[0] = grads[m]


def body(tokens, out_grad, expert_ids, probs, w_gate, w_up, w_down):
    vmem = pl.BlockSpec(memory_space=pltpu.VMEM)
    hbm = pl.BlockSpec(memory_space=pltpu.HBM)
    grads = jax.ShapeDtypeStruct((1, 128, FF), F32)
    token_grad = jax.ShapeDtypeStruct(tokens.shape, BF16)
    small = probs.T.shape
    dma = pltpu.SemaphoreType.DMA
    held = (tokens, out_grad, expert_ids.T, probs.T, w_gate, w_up, w_down)
    stay = [pltpu.with_memory_space_constraint(a, pltpu.HBM) for a in held]
    sums = pl.pallas_call(
        kernel,
        out_shape=(token_grad, jax.ShapeDtypeStruct(small, F32), jax.ShapeDtypeStruct((3, 128, FF), F32)),
        in_specs=[hbm] * 7,
        out_specs=(vmem,) * 3,
        scratch_shapes=[
            pltpu.VMEM(small, jnp.int32),
            pltpu.VMEM(small, BF16),
            pltpu.VMEM((2, N * TOK, D + EXTRA), BF16),
            pltpu.VMEM((2, ROWS, D + EXTRA), BF16),
            pltpu.VMEM((2, ROWS, D + EXTRA), BF16),
            pltpu.VMEM((D, 2 * FF), BF16),
            pltpu.VMEM((D, FF), BF16),
            pltpu.VMEM((ROWS, 3 * FF), F32),
            pltpu.VMEM((ROWS, D), BF16),
            pltpu.VMEM((ROWS, 2 * FF), BF16),
            pltpu.VMEM((ROWS, 2 * FF), BF16),
            pltpu.VMEM((ROWS, FF), BF16),
            pltpu.VMEM((2, ROWS, HALF + EXTRA), BF16),
            pltpu.VMEM((2, ROWS, HALF + EXTRA), BF16),
            pltpu.VMEM((2, N * TOK, HALF + EXTRA), BF16),
            pltpu.VMEM((2, N * TOK, HALF + EXTRA), BF16),
            pltpu.VMEM((N, 2, 3, 128, FF), BF16),
            pltpu.VMEM((N, 3, 128, FF), BF16),
            pltpu.VMEM((2, 3, 3, 128, FF), BF16),
            pltpu.VMEM((2, 3, 3, 128, FF), BF16),
            pltpu.VMEM((2, 3, 64, FF), BF16),
            pltpu.VMEM((2, 3, 64, FF), BF16),
            dma((4,)),
            dma((3,)),
            dma((2, N)), dma((2, N)),
            dma((2, GROUPS, N - 1)), dma((2, GROUPS, N - 1)),
            dma((2, N - 1)), dma((2, N - 1)),
            dma((2, N - 1)), dma((2, N - 1)),
            dma((N,)), dma((N,)),
            dma((2, 4, 3)), dma((2, 4, 3)),
        ],
        compiler_params=pltpu.CompilerParams(collective_id=0, has_side_effects=True, vmem_limit_bytes=VMEM_LIMIT),
        name="expert_layer_backward",
    )(*stay)
    token_grad, prob_grad, *weight_grads = pl.pallas_call(
        finish,
        out_shape=(token_grad, jax.ShapeDtypeStruct(small, BF16), grads, grads, grads),
        in_specs=[vmem] * 3,
        out_specs=(vmem,) * 5,
        compiler_params=pltpu.CompilerParams(vmem_limit_bytes=4 << 20),
        name="write_outputs",
    )(*sums)
    return (token_grad, prob_grad.T, *weight_grads)


def solution(mesh):
    rows = P(("dp", "expert"), None)
    weights = P("expert", None, None)
    grads = P("expert", "dp", None)
    return jax.shard_map(
        body,
        mesh=mesh,
        in_specs=(rows, rows, rows, rows, weights, weights, weights),
        out_specs=(rows, rows, grads, grads, grads),
        check_vma=False,
    )
```

```python
import jax
import jax.numpy as jnp
from jax import lax
from jax.experimental import pallas as pl
from jax.experimental.pallas import tpu as pltpu
from jax.sharding import PartitionSpec as P

MESH = pl.DeviceIdType.MESH
F32, BF16 = jnp.float32, jnp.bfloat16
N = 8
OFF = (0, 1, 7, 2, 6, 3, 5, 4)
TOK, SLOT, D, FF, EXTRA = 16, 4, 2048, 384, 128
ROWS = N * N * SLOT
HALF = D // 2
GROUPS = 2
VMEM_LIMIT = 209 << 18
PER = N // GROUPS
CHUNKS = 2


def dot(a, b, ca=1, cb=0):
    return lax.dot_general(a, b, (((ca,), (cb,)), ((), ())), preferred_element_type=F32)


def iota(shape, axis):
    return lax.broadcasted_iota(jnp.int32, shape, axis)


def offset_of(k):
    return jnp.where(k % 2 == 1, (k + 1) // 2, (N - k // 2) % N)


def codes(weights):
    n = weights.shape[0]
    mask = weights.astype(F32) > 0.0
    r, c = iota((n, n), 0), iota((n, n), 1)
    before = jnp.where((r // TOK == c // TOK) & (c < r), 1.0, 0.0).astype(BF16)
    place = dot(before, jnp.where(mask, 1.0, 0.0).astype(BF16))
    return jnp.where(mask, place + 1.0, 0.0).astype(BF16)


def expert_lane(side, z, y, k):
    if side == 0:
        return z * N + (y + offset_of(k)) % N
    return ((z + offset_of(k)) % N) * N + y


def kernel(
    tok_h, dy_h, ids_h, pr_h, wg_h, wu_h, wd_h,
    tg_out, pg_out, grads_out,
    ids, pr, gather, send2, recv2, wgu, wd, gu, dyr, gbub, gbub_b, pact,
    contrib, back, tpart, trecv, part, other, ring_s, ring_r, ring1_s, ring1_r,
    isem, wsem, p1s, p1r, p2s, p2r, c1s, c1r, c2s, c2r, ds, dr, rs, rr,
):
    dp, ex = lax.axis_index("dp"), lax.axis_index("expert")
    x, core = dp // 2, dp % 2
    z, y = ex // N, ex % N

    def along(side, d):
        if side == 0:
            return (dp, ((z + d) % N) * N + y)
        return (dp, z * N + (y + d) % N)

    ahead = (((x + 1) % N) * 2 + core, ex)
    behind = (((x + N - 1) % N) * 2 + core, ex)
    partner = (x * 2 + 1 - core, ex)

    inputs = [
        pltpu.make_async_copy(src, dst, isem.at[i])
        for i, (src, dst) in enumerate((
            (ids_h, ids), (pr_h, pr),
            (tok_h, gather.at[0, pl.ds(0, TOK), pl.ds(0, D)]), (dy_h, gather.at[1, pl.ds(0, TOK), pl.ds(0, D)]),
        ))
    ]
    for load in inputs:
        load.start()
    loads = [
        pltpu.make_async_copy(wg_h.at[0], wgu.at[:, pl.ds(0, FF)], wsem.at[0]),
        pltpu.make_async_copy(wu_h.at[0], wgu.at[:, pl.ds(FF, FF)], wsem.at[1]),
        pltpu.make_async_copy(wd_h.at[0], wd, wsem.at[2]),
    ]
    for load in loads:
        load.start()

    barrier = pltpu.get_barrier_semaphore()
    peers = [along(side, d) for d in range(1, N) for side in range(2)] + [ahead, behind, partner]
    for peer in peers:
        pl.semaphore_signal(barrier, inc=1, device_id=peer, device_id_type=MESH)

    for load in inputs:
        load.wait()
    top = ids.shape[0]
    wide = pr[...].astype(F32)
    expert = iota((EXTRA, TOK), 0)
    dense = jnp.zeros((EXTRA, TOK), F32)
    for k in range(top):
        dense += jnp.where(expert == ids[k : k + 1, :], wide[k : k + 1, :], 0.0)
    dense = dense.T.astype(BF16)
    for side in range(2):
        gather[side, 0:TOK, D : D + EXTRA] = dense

    pl.semaphore_wait(barrier, len(peers))

    sends = []

    def remote(src, dst, ssem, rsem, device):
        return pltpu.make_async_remote_copy(
            src_ref=src, dst_ref=dst, send_sem=ssem, recv_sem=rsem, device_id=device, device_id_type=MESH
        )

    def start(copy):
        copy.start()
        sends.append(copy)
        return copy

    def share(side, i, src_slab, dst_slab, d, cols):
        src, dst = (gather.at[side, pl.ds(TOK * k, TOK), cols] for k in (src_slab, dst_slab))
        return start(remote(src, dst, p1s.at[side, i], p1r.at[side, i], along(side, d % N)))

    every = pl.ds(0, D + EXTRA)
    first, second = pl.ds(0, HALF), pl.ds(HALF, HALF + EXTRA)
    hop1 = [[[] for _ in range(N)] for _ in range(2)]
    for k in (3, 4, 1, 2):
        for side in range(2):
            hop1[side][k].append(share(side, k - 1, 0, k, OFF[k], every))
    for slab, to, d, i, cols in ((3, 5, 1, 6, first), (4, 6, -1, 7, second)):
        for side in range(2):
            for copy in hop1[side][slab]:
                copy.wait_recv()
            hop1[side][slab] = []
            hop1[side][to].append(share(side, to - 1, slab, to, d, every))
            hop1[side][N - 1].append(share(side, i, slab, N - 1, 2 * d, cols))

    width = (D + EXTRA, D)
    hop2 = []
    for g in range(GROUPS):
        n_tok, n_row = PER * TOK, N * PER * SLOT
        for side in range(2):
            for k in range(g * PER, (g + 1) * PER):
                for copy in hop1[side][k]:
                    copy.wait_recv()
            rows_at = pl.ds(g * n_tok, n_tok)
            code = codes(gather[side, rows_at, D : D + EXTRA])
            r, c = iota((n_row, EXTRA), 0), iota((n_row, EXTRA), 1)
            pick = jnp.where(c == expert_lane(side, z, y, r // (PER * SLOT)), 1.0, 0.0).astype(BF16)
            found = dot(pick, code, 1, 1)
            r, c = iota((n_row, n_tok), 0), iota((n_row, n_tok), 1)
            hit = (found == (r % SLOT + 1).astype(F32)) & ((r // SLOT) % PER == c // TOK)
            sel = jnp.where(hit, 1.0, 0.0).astype(BF16)

            def choose(cols, side=side, sel=sel, rows_at=rows_at, g=g):
                rows = dot(sel, gather[side, rows_at, cols]).astype(BF16)
                m = PER * SLOT
                for k in range(N):
                    target = send2 if k else recv2
                    target[side, pl.ds(k * N * SLOT + g * m, m), cols] = rows[k * m : (k + 1) * m]

            def tile(n, carry, choose=choose):
                choose(pl.ds(pl.multiple_of(n * 256, 256), 256))
                return carry

            lax.fori_loop(0, D // 256, tile, 0)
            if side == 0:
                choose(pl.ds(D, EXTRA))
            m = PER * SLOT
            for k in range(N - 1, 0, -1):
                at = pl.ds(k * N * SLOT + g * m, m)
                cols = pl.ds(0, width[side])
                hop2.append(
                    start(
                        remote(
                            send2.at[side, at, cols], recv2.at[side, at, cols],
                            p2s.at[side, g, k - 1], p2r.at[side, g, k - 1], along(1 - side, OFF[k]),
                        )
                    )
                )

    r, c = iota((ROWS, EXTRA), 0), iota((ROWS, EXTRA), 1)
    t, q = iota((N * TOK, ROWS), 0), iota((N * TOK, ROWS), 1)
    gives = []
    for side in range(2):
        code = codes(gather[side, :, D : D + EXTRA])
        pick = jnp.where(c == expert_lane(side, z, y, r // (N * SLOT)), 1.0, 0.0).astype(BF16)
        found = dot(code, pick, 1, 1)
        hit = (found == (q % SLOT + 1).astype(F32)) & ((q // SLOT) % N == t // TOK)
        gives.append(jnp.where(hit, 1.0, 0.0).astype(BF16))
    r, c = iota((ROWS, ROWS), 0), iota((ROWS, ROWS), 1)
    swapped = ((r // SLOT) % N) * (N * SLOT) + (r // (N * SLOT)) * SLOT + r % SLOT
    swap = jnp.where(c == swapped, 1.0, 0.0).astype(BF16)

    for load in loads:
        load.wait()
    for copy in hop2:
        copy.wait_recv()

    def tile_gu(n, carry):
        cols = pl.ds(pl.multiple_of(n * 256, 256), 256)
        gu[:, cols] = dot(recv2[0, :, 0:D], wgu[:, cols])
        return carry

    lax.fori_loop(0, 2 * FF // 256, tile_gu, 0)

    def tile_swap(n, carry):
        cols = pl.ds(pl.multiple_of(n * 256, 256), 256)
        dyr[:, cols] = dot(swap, recv2[1, :, cols]).astype(BF16)
        return carry

    lax.fori_loop(0, D // 256, tile_swap, 0)
    gu[:, 2 * FF : 3 * FF] = dot(dyr[...], wd[...])

    chunk = 32

    def middle(n, carry):
        at = pl.ds(pl.multiple_of(n * chunk, chunk), chunk)
        lane = iota((chunk, EXTRA), 1)
        p = jnp.sum(jnp.where(lane == ex, recv2[0, at, D : D + EXTRA].astype(F32), 0.0), axis=1, keepdims=True)
        gate, up, dyw = gu[at, 0:FF], gu[at, FF : 2 * FF], gu[at, 2 * FF : 3 * FF]
        sigma = 1.0 / (1.0 + jnp.exp(-gate))
        silu = gate * sigma
        act = (silu * up).astype(BF16).astype(F32)
        prob_back = jnp.sum(act * dyw, axis=1, keepdims=True)
        contrib[0, at, HALF : HALF + EXTRA] = jnp.where(lane == ex, prob_back, 0.0).astype(BF16)
        act_grad = p * dyw
        gbub[at, 0:FF] = (act_grad * up * sigma * (1.0 + gate * (1.0 - sigma))).astype(BF16)
        gbub[at, FF : 2 * FF] = (act_grad * silu).astype(BF16)
        pact[at, :] = (p * act).astype(BF16)
        return carry

    lax.fori_loop(0, ROWS // chunk, middle, 0)

    swap_core = {}

    def shards(n):
        cols = pl.ds(pl.multiple_of(((x + n) % N) * 256, 256), 256)
        both = dot(recv2[0, :, cols], gbub[...], 0, 0).astype(BF16)
        down = dot(dyr[:, cols], pact[...], 0, 0).astype(BF16)
        for h in range(2):
            rows = slice(h * 128, h * 128 + 128)
            part[n, h, 0] = both[rows, 0:FF]
            part[n, h, 1] = both[rows, FF : 2 * FF]
            part[n, h, 2] = down[rows]
        swap_core[n] = start(remote(part.at[n, 1 - core], other.at[n], ds.at[n], dr.at[n], partner))

    def chip(m, rel, rows=pl.ds(0, 128)):
        return part[rel, core, m, rows, :].astype(F32) + other[rel, m, rows, :].astype(F32)

    line, wide_cols = N * SLOT, HALF // CHUNKS

    def chunk_cols(side, ch):
        last = EXTRA if side == 0 and ch == CHUNKS - 1 else 0
        return pl.ds(ch * wide_cols, wide_cols + last)

    back1 = {}

    def send_back(side, ch):
        mine = gbub if side == 0 else gbub_b
        for n in range(wide_cols // 256):
            at = ch * wide_cols + n * 256
            weights = wgu[side * HALF + at : side * HALF + at + 256, :]
            contrib[side, :, at : at + 256] = dot(mine[...], weights, 1, 1).astype(BF16)
        cols = chunk_cols(side, ch)
        for k in range(N - 1, 0, -1):
            at = pl.ds(k * line, line)
            back1[side, ch, k] = start(
                remote(
                    contrib.at[side, at, cols], back.at[side, at, cols],
                    c1s.at[side, ch, k - 1], c1r.at[side, ch, k - 1], along(1 - side, N - OFF[k]),
                )
            )
        back[side, 0:line, cols] = contrib[side, 0:line, cols]

    back2 = []

    def send_home(side, ch):
        for k in range(1, N):
            back1[side, ch, k].wait_recv()
        cols = chunk_cols(side, ch)
        tpart[side, :, cols] = dot(gives[side], back[side, :, cols]).astype(BF16)
        for k in range(N - 1, 0, -1):
            at = pl.ds(k * TOK, TOK)
            back2.append(
                start(
                    remote(
                        tpart.at[side, at, cols], trecv.at[side, at, cols],
                        c2s.at[side, ch, k - 1], c2r.at[side, ch, k - 1], along(side, N - OFF[k]),
                    )
                )
            )
        trecv[side, 0:TOK, cols] = tpart[side, 0:TOK, cols]

    shards(4)
    send_back(0, 0)
    gbub_b[...] = dot(swap, gbub[...]).astype(BF16)
    send_back(1, 0)

    towards = (ahead, behind)
    halves = (pl.ds(0, 64), pl.ds(64, 64))
    ring = {}
    swap_core[4].wait_recv()
    for m in range(3):
        for w in range(2):
            ring1_s[w, m] = chip(m, 4, halves[w]).astype(BF16)
            ring[w, 0, m] = start(
                remote(ring1_s.at[w, m], ring1_r.at[w, m], rs.at[w, 0, m], rr.at[w, 0, m], towards[w])
            )

    for n in (3, 5):
        shards(n)
    for ch in range(1, CHUNKS):
        for side in range(2):
            send_back(side, ch)

    def ring_step(step):
        swap_core[4 - step].wait_recv()
        swap_core[4 + step].wait_recv()
        for m in range(3):
            for w in range(2):
                rel = 4 - step if w == 0 else 4 + step
                ring[w, step - 1, m].wait_recv()
                if step == 1:
                    a, b = halves[w], halves[1 - w]
                    ring_s[w, 0, m, a, :] = (chip(m, rel, a) + ring1_r[w, m].astype(F32)).astype(BF16)
                    ring_s[w, 0, m, b, :] = chip(m, rel, b).astype(BF16)
                else:
                    ring_s[w, step - 1, m] = (chip(m, rel) + ring_r[w, step - 2, m].astype(F32)).astype(BF16)
                ring[w, step, m] = start(
                    remote(
                        ring_s.at[w, step - 1, m], ring_r.at[w, step - 1, m],
                        rs.at[w, step, m], rr.at[w, step, m], towards[w],
                    )
                )

    ring_step(1)
    for n in (2, 6, 1, 7, 0):
        shards(n)
    ring_step(2)
    for side in range(2):
        send_home(side, 0)
    ring_step(3)
    for ch in range(1, CHUNKS):
        for side in range(2):
            send_home(side, ch)

    for copy in back2:
        copy.wait_recv()
    for side in range(2):
        total = jnp.zeros((TOK, HALF), F32)
        for k in range(N):
            total += trecv[side, k * TOK : (k + 1) * TOK, 0:HALF].astype(F32)
        tg_out[:, side * HALF : (side + 1) * HALF] = total.astype(BF16)
    dense = jnp.zeros((TOK, EXTRA), F32)
    for k in range(N):
        dense += trecv[0, k * TOK : (k + 1) * TOK, HALF : HALF + EXTRA].astype(F32)
    dense = dense.T
    for k in range(top):
        one = jnp.where(expert == ids[k : k + 1, :], dense, 0.0)
        pg_out[k : k + 1, :] = jnp.sum(one, axis=0, keepdims=True)

    swap_core[0].wait_recv()
    for m in range(3):
        ring[0, 3, m].wait_recv()
        ring[1, 3, m].wait_recv()
        grads_out[m] = chip(m, 0) + ring_r[0, 2, m].astype(F32) + ring_r[1, 2, m].astype(F32)

    for copy in sends:
        copy.wait_send()


def finish(tg, pg, grads, tg_out, pg_out, gg_out, ug_out, dg_out):
    tg_out[...] = tg[...]
    pg_out[...] = pg[...].astype(BF16)
    for m, out in enumerate((gg_out, ug_out, dg_out)):
        out[0] = grads[m]


def body(tokens, out_grad, expert_ids, probs, w_gate, w_up, w_down):
    vmem = pl.BlockSpec(memory_space=pltpu.VMEM)
    hbm = pl.BlockSpec(memory_space=pltpu.HBM)
    grads = jax.ShapeDtypeStruct((1, 128, FF), F32)
    token_grad = jax.ShapeDtypeStruct(tokens.shape, BF16)
    small = probs.T.shape
    dma = pltpu.SemaphoreType.DMA
    held = (tokens, out_grad, expert_ids.T, probs.T, w_gate, w_up, w_down)
    stay = [pltpu.with_memory_space_constraint(a, pltpu.HBM) for a in held]
    sums = pl.pallas_call(
        kernel,
        out_shape=(token_grad, jax.ShapeDtypeStruct(small, F32), jax.ShapeDtypeStruct((3, 128, FF), F32)),
        in_specs=[hbm] * 7,
        out_specs=(vmem,) * 3,
        scratch_shapes=[
            pltpu.VMEM(small, jnp.int32),
            pltpu.VMEM(small, BF16),
            pltpu.VMEM((2, N * TOK, D + EXTRA), BF16),
            pltpu.VMEM((2, ROWS, D + EXTRA), BF16),
            pltpu.VMEM((2, ROWS, D + EXTRA), BF16),
            pltpu.VMEM((D, 2 * FF), BF16),
            pltpu.VMEM((D, FF), BF16),
            pltpu.VMEM((ROWS, 3 * FF), F32),
            pltpu.VMEM((ROWS, D), BF16),
            pltpu.VMEM((ROWS, 2 * FF), BF16),
            pltpu.VMEM((ROWS, 2 * FF), BF16),
            pltpu.VMEM((ROWS, FF), BF16),
            pltpu.VMEM((2, ROWS, HALF + EXTRA), BF16),
            pltpu.VMEM((2, ROWS, HALF + EXTRA), BF16),
            pltpu.VMEM((2, N * TOK, HALF + EXTRA), BF16),
            pltpu.VMEM((2, N * TOK, HALF + EXTRA), BF16),
            pltpu.VMEM((N, 2, 3, 128, FF), BF16),
            pltpu.VMEM((N, 3, 128, FF), BF16),
            pltpu.VMEM((2, 3, 3, 128, FF), BF16),
            pltpu.VMEM((2, 3, 3, 128, FF), BF16),
            pltpu.VMEM((2, 3, 64, FF), BF16),
            pltpu.VMEM((2, 3, 64, FF), BF16),
            dma((4,)),
            dma((3,)),
            dma((2, N)), dma((2, N)),
            dma((2, GROUPS, N - 1)), dma((2, GROUPS, N - 1)),
            dma((2, CHUNKS, N - 1)), dma((2, CHUNKS, N - 1)),
            dma((2, CHUNKS, N - 1)), dma((2, CHUNKS, N - 1)),
            dma((N,)), dma((N,)),
            dma((2, 4, 3)), dma((2, 4, 3)),
        ],
        compiler_params=pltpu.CompilerParams(collective_id=0, has_side_effects=True, vmem_limit_bytes=VMEM_LIMIT),
        name="expert_layer_backward",
    )(*stay)
    token_grad, prob_grad, *weight_grads = pl.pallas_call(
        finish,
        out_shape=(token_grad, jax.ShapeDtypeStruct(small, BF16), grads, grads, grads),
        in_specs=[vmem] * 3,
        out_specs=(vmem,) * 5,
        compiler_params=pltpu.CompilerParams(vmem_limit_bytes=4 << 20),
        name="write_outputs",
    )(*sums)
    return (token_grad, prob_grad.T, *weight_grads)


def solution(mesh):
    rows = P(("dp", "expert"), None)
    weights = P("expert", None, None)
    grads = P("expert", "dp", None)
    return jax.shard_map(
        body,
        mesh=mesh,
        in_specs=(rows, rows, rows, rows, weights, weights, weights),
        out_specs=(rows, rows, grads, grads, grads),
        check_vma=False,
    )
```
